32 devices in a mesh: kv: 16 (over z, y, core), batch: 2 (over x).
Axes of the slice: x: 2, y: 2, z: 4, core: 2. Of those that a mesh axis runs over, the one named last changes fastest.
Arguments:
- queries: bfloat16 [32, 4, 32, 128], P(('kv', 'batch')), may hold values from -200 to 200
- prefix_keys: bfloat16 [2048, 16, 128], P(('kv', 'batch')), may hold values from -12 to 12
- prefix_values: bfloat16 [2048, 16, 128], P(('kv', 'batch')), may hold values from -12 to 12
- suffix_keys: bfloat16 [32, 1024, 16, 128], P(('kv', 'batch')), may hold values from -14 to 14
- suffix_values: bfloat16 [32, 1024, 16, 128], P(('kv', 'batch')), may hold values from -12 to 12
- lengths: int32 [32], P(('kv', 'batch')), may hold values from 256 to 1024, as said below
Outputs:
- attended: bfloat16 [32, 4, 32, 128], P(('kv', 'batch'))
The draws below stay inside these ranges and needn't reach their ends.
Inputs may be any that keep to these rules, and one draw needn't show every extreme that they name: `lengths`: each sequence's own cache holds its 4 new tokens in its last used slots; some sequence fills all 1024 slots.
All inputs are finite; a program needn't handle non-finite values.
Results may differ from the reference program's by a relative error of at most 0.0045.
Values may be sent and summed in bfloat16 or wider, within the bound.
A program may use at most 64 MiB of HBM per device.

```python
import jax
import jax.numpy as jnp
from jax import lax

QH = 32
KV_HEADS = 16
HEAD_WIDTH = 128
QUERY_SCALE = 144
NEW_QUERY_COUNT = 4
SUFFIX = 1024
PREFIX_DEV = 64
SEQUENCE_COUNT = 32
PREFIX = 2048


def prompt_key_core(key):
    base = jax.random.normal(jax.random.fold_in(key, 101), (PREFIX, KV_HEADS, HEAD_WIDTH), jnp.float32)
    shifts = jax.random.normal(jax.random.fold_in(key, 102), (PREFIX // PREFIX_DEV, KV_HEADS, HEAD_WIDTH), jnp.float32) * 1.5
    return jnp.clip(base + jnp.repeat(shifts, PREFIX_DEV, axis=0), -12.0, 12.0)


def draw_prefix_keys(key, part):
    return prompt_key_core(key).astype(jnp.bfloat16)


def draw_prefix_values(key, part):
    base = jax.random.normal(jax.random.fold_in(key, 111), (PREFIX, KV_HEADS, HEAD_WIDTH), jnp.float32)
    shifts = jax.random.normal(jax.random.fold_in(key, 112), (PREFIX // PREFIX_DEV, KV_HEADS, HEAD_WIDTH), jnp.float32) * 2.0
    return jnp.clip(base + jnp.repeat(shifts, PREFIX_DEV, axis=0), -12.0, 12.0).astype(jnp.bfloat16)


def draw_queries(key, part):
    factor = 1.5
    values = jax.random.normal(jax.random.fold_in(key, 103), (SEQUENCE_COUNT, NEW_QUERY_COUNT, QH, HEAD_WIDTH), jnp.float32)
    values = jnp.clip(values, -6.0, 6.0) * factor
    prompt = prompt_key_core(key).astype(jnp.bfloat16).astype(jnp.float32)
    chosen = jax.random.randint(jax.random.fold_in(key, 104), (6,), 0, SEQUENCE_COUNT)
    first_pos = jax.random.randint(jax.random.fold_in(key, 105), (6,), 0, PREFIX)
    second_pos = jax.random.randint(jax.random.fold_in(key, 106), (6,), 0, PREFIX)
    levels = jnp.array([4.5, 3.0, 1.5, 3.0, 4.5, 1.5], jnp.float32)
    strength = levels * (512.0 / HEAD_WIDTH)
    paired = (prompt[first_pos] + prompt[second_pos]) * 0.5
    paired = jnp.repeat(paired, QH // KV_HEADS, axis=1)
    values = values.at[chosen, 0].set(strength[:, None, None] * paired)
    return jnp.clip(values, -200.0, 200.0).astype(jnp.bfloat16)


def draw_lengths(key, part):
    drawn = jax.random.randint(jax.random.fold_in(key, 107), (SEQUENCE_COUNT,), SUFFIX // 4, SUFFIX + 1)
    fullest = jax.random.randint(jax.random.fold_in(key, 108), (), 0, SEQUENCE_COUNT)
    return drawn.at[fullest].set(SUFFIX).astype(jnp.int32)


def level_of(own_key, dims, pieces, smallest, top_value):
    def one(position, parts):
        draws = jax.random.uniform(jax.random.fold_in(jax.random.fold_in(own_key, 6), position), (parts,), jnp.float32, smallest / len(pieces), top_value / len(pieces))
        return jnp.repeat(jnp.exp(draws), dims[position] // parts).reshape((-1,) + (1,) * (len(dims) - position - 1))

    loudness = one(*pieces[0])
    for cut in pieces[1:]:
        loudness = loudness * one(*cut)
    return loudness


def gaussian(stream_key, extent, width, reach, cuts=(), kind=jnp.bfloat16):
    loudness = level_of(stream_key, extent, cuts, -0.22, 0.18) if cuts else 1.0
    values = jax.random.normal(stream_key, extent, jnp.float32) * width * loudness
    return jnp.minimum(jnp.maximum(values, -reach), reach).astype(kind)


def setup_inputs(seed: int = 0) -> dict:
    arg_keys = jax.random.split(jax.random.key(seed), 7)
    queries = draw_queries(jax.random.fold_in(arg_keys[6], 71), 0)
    prefix_keys = draw_prefix_keys(jax.random.fold_in(arg_keys[6], 71), 0)
    prefix_values = draw_prefix_values(jax.random.fold_in(arg_keys[6], 71), 0)
    suffix_keys = gaussian(arg_keys[3], (SEQUENCE_COUNT, SUFFIX, KV_HEADS, HEAD_WIDTH), 2.5, 14.0, ((0, 32),))
    suffix_values = gaussian(arg_keys[4], (SEQUENCE_COUNT, SUFFIX, KV_HEADS, HEAD_WIDTH), 2.5, 12.0, ((0, 32),))
    lengths = draw_lengths(jax.random.fold_in(arg_keys[6], 71), 0)
    return {"queries": queries, "prefix_keys": prefix_keys, "prefix_values": prefix_values, "suffix_keys": suffix_keys, "suffix_values": suffix_values, "lengths": lengths}


masked_score = -1.0e30


def reference(queries, prefix_keys, prefix_values, suffix_keys, suffix_values, lengths):
    scaling = QUERY_SCALE ** -0.5
    queries_per_group = QH // KV_HEADS
    grouped = queries.reshape(SEQUENCE_COUNT, NEW_QUERY_COUNT, KV_HEADS, queries_per_group, HEAD_WIDTH)
    limits = lengths[:, None] - NEW_QUERY_COUNT + 1 + jnp.arange(NEW_QUERY_COUNT, dtype=jnp.int32)[None, :]
    limits = jnp.repeat(limits, queries_per_group, axis=1)
    positions = jnp.arange(SUFFIX, dtype=jnp.int32)
    visible = positions[None, None, :] < limits[:, :, None]

    def one_head(head):
        query_rows = lax.dynamic_index_in_dim(grouped, head, 2, keepdims=False)
        keys_prompt = lax.dynamic_index_in_dim(prefix_keys, head, 1, keepdims=False)
        values_prompt = lax.dynamic_index_in_dim(prefix_values, head, 1, keepdims=False)
        keys_own = lax.dynamic_index_in_dim(suffix_keys, head, 2, keepdims=False)
        suffix_value_rows = lax.dynamic_index_in_dim(suffix_values, head, 2, keepdims=False)
        flat_rows = query_rows.reshape(SEQUENCE_COUNT * NEW_QUERY_COUNT * queries_per_group, HEAD_WIDTH)
        prompt_scores = jnp.dot(flat_rows, keys_prompt.T, preferred_element_type=jnp.float32) * scaling
        prompt_scores = prompt_scores.reshape(SEQUENCE_COUNT, NEW_QUERY_COUNT * queries_per_group, PREFIX)
        suffix_scores = jnp.einsum("ixv,iav->ixa", query_rows.reshape(SEQUENCE_COUNT, NEW_QUERY_COUNT * queries_per_group, HEAD_WIDTH).astype(jnp.float32),
                                keys_own.astype(jnp.float32)) * scaling
        suffix_scores = jnp.where(visible, suffix_scores, masked_score)
        top = jnp.maximum(jnp.max(prompt_scores, -1), jnp.max(suffix_scores, -1))
        prompt_weights = jnp.exp(prompt_scores - top[..., None])
        own_weights = jnp.exp(suffix_scores - top[..., None])
        total = jnp.sum(prompt_weights, -1) + jnp.sum(own_weights, -1)
        prompt_rounded = prompt_weights.astype(jnp.bfloat16).reshape(SEQUENCE_COUNT * NEW_QUERY_COUNT * queries_per_group, PREFIX)
        prompt_part = jnp.dot(prompt_rounded, values_prompt, preferred_element_type=jnp.float32)
        prompt_part = prompt_part.reshape(SEQUENCE_COUNT, NEW_QUERY_COUNT * queries_per_group, HEAD_WIDTH)
        suffix_rounded = lax.optimization_barrier(own_weights.astype(jnp.bfloat16))
        suffix_partial = jnp.einsum("caj,cjv->cav", suffix_rounded.astype(jnp.float32), suffix_value_rows.astype(jnp.float32))
        result = (prompt_part + suffix_partial) / total[..., None]
        return result.reshape(SEQUENCE_COUNT, NEW_QUERY_COUNT, queries_per_group, HEAD_WIDTH)

    outputs = lax.map(one_head, jnp.arange(KV_HEADS, dtype=jnp.int32))
    outputs = jnp.moveaxis(outputs, 0, 2)
    return outputs.reshape(SEQUENCE_COUNT, NEW_QUERY_COUNT, QH, HEAD_WIDTH).astype(jnp.bfloat16)
```

```python
import functools

import jax
import jax.numpy as jnp
from jax import lax
from jax.experimental import pallas as pl
from jax.experimental.pallas import tpu as pltpu
from jax.sharding import PartitionSpec as P

QUERY_SCALE = 144
MESH = pl.DeviceIdType.MESH
masked_score = -1e30
CHUNKS = 8


def dot_nt(a, b):
    return lax.dot_general(a, b, (((1,), (1,)), ((), ())), preferred_element_type=jnp.float32)


def kernel(
    sizes, length, q_hbm, kv_hbm, sk_hbm, sv_hbm, out_ref,
    qs, ks, vs, times, qa, qb, kva, kvb, oa, ob, la, lb, ra, rb, sa, sb,
    suffix_sem, local_sem, qa_send, qa_recv, qb_send, qb_recv,
    core_send, core_recv, xa_send, xa_recv, fa_send, fa_recv, yb_send, yb_recv,
    fb_send, fb_recv, oa_send, oa_recv, ob_send, ob_recv,
    la_send, la_recv, lb_send, lb_recv,
):
    deep, wide, new_tokens, rows, half, count_p, depth, kv_heads = sizes
    kv, x = lax.axis_index("kv"), lax.axis_index("batch")
    core, zy = kv % 2, kv // 2
    y, z = zy % 2, zy // 2
    na, nb = 2 * deep, deep * wide
    ia, ib = zy, z * wide + x
    scaling = QUERY_SCALE ** (-0.5)

    def device_a(i):
        return (i * 2 + core, x)

    def device_b(i):
        return ((i // wide * 2 + y) * 2 + core, i % wide)

    sibling = (kv + 1 - 2 * core, x)
    slot_a, slot_b = x * 2 + core, y * 2 + core

    locals_ = [
        pltpu.make_async_copy(q_hbm.at[0], qa.at[ia], local_sem.at[0]),
        pltpu.make_async_copy(q_hbm.at[1], qb.at[ib], local_sem.at[1]),
        pltpu.make_async_copy(kv_hbm.at[0], kva.at[slot_a], local_sem.at[2]),
        pltpu.make_async_copy(kv_hbm.at[1], kvb.at[slot_b], local_sem.at[3]),
        pltpu.make_async_copy(q_hbm, qs, local_sem.at[4]),
    ]
    for copy in locals_:
        copy.start()
    span = ks.shape[0] // CHUNKS
    loads = []
    for c in range(CHUNKS):
        part = pl.ds(c * span, span)
        loads.append((
            pltpu.make_async_copy(sk_hbm.at[part], ks.at[part], suffix_sem.at[0, c]),
            pltpu.make_async_copy(sv_hbm.at[part], vs.at[part], suffix_sem.at[1, c]),
        ))
        for copy in loads[-1]:
            copy.start()

    barrier = pltpu.get_barrier_semaphore()

    def peers(n, me, act):
        def step(k, carry):
            act(lax.rem(me + k, n))
            return carry

        lax.fori_loop(1, n, step, 0, unroll=n <= 16)

    def greet(device):
        pl.semaphore_signal(barrier, inc=1, device_id=device, device_id_type=MESH)

    greet(sibling)
    peers(na, ia, lambda i: greet(device_a(i)))
    peers(nb, ib, lambda i: greet(device_b(i)))
    pl.semaphore_wait(barrier, na + nb - 1)

    def remote(src, dst, send, recv, device):
        return pltpu.make_async_remote_copy(
            src_ref=src, dst_ref=dst, send_sem=send, recv_sem=recv,
            device_id=device, device_id_type=MESH,
        )

    for copy in locals_:
        copy.wait()
    q_a = lambda i, s: remote(qa.at[s], qa.at[s], qa_send.at[i], qa_recv.at[s], device_a(i))
    q_b = lambda i, s: remote(qb.at[s], qb.at[s], qb_send.at[i], qb_recv.at[s], device_b(i))
    peers(na, ia, lambda i: q_a(i, ia).start())
    peers(nb, ib, lambda i: q_b(i, ib).start())
    x_a = lambda i, s: remote(
        kva.at[s], kva.at[s], xa_send.at[i], xa_recv.at[s // 2], (kv, i))
    peers(wide, x, lambda i: x_a(i, slot_a).start())
    y_b = lambda s: remote(
        kvb.at[s], kvb.at[s], yb_send, yb_recv, ((z * 2 + 1 - y) * 2 + core, x))
    y_b(slot_b).start()
    c_a = lambda s: remote(kva.at[s], kva.at[s], core_send.at[0], core_recv.at[0], sibling)
    c_b = lambda s: remote(kvb.at[s], kvb.at[s], core_send.at[1], core_recv.at[1], sibling)
    c_a(slot_a).start()
    c_b(slot_b).start()

    total_rows = kv_heads * rows
    row = lax.broadcasted_iota(jnp.int32, (total_rows, span), 0)
    col = lax.broadcasted_iota(jnp.int32, (total_rows, span), 1)
    times[...] = jnp.where(row // rows == col % kv_heads, col // kv_heads, 2 ** 30)
    token = lax.broadcasted_iota(jnp.int32, (total_rows, 1), 0) % rows // (rows // new_tokens)
    limit = length[0] - new_tokens + 1 + token
    queries = jnp.concatenate([qs[0], qs[1]], axis=0)
    top = jnp.full((total_rows, 1), masked_score, jnp.float32)
    total = jnp.zeros((total_rows, 1), jnp.float32)
    acc = jnp.zeros((total_rows, depth), jnp.float32)
    for c in range(CHUNKS):
        for copy in loads[c]:
            copy.wait()
        part = pl.ds(c * span, span)
        scores = dot_nt(queries, ks[part]) * scaling
        scores = jnp.where(times[...] < limit - c * (span // kv_heads), scores, masked_score)
        higher = jnp.maximum(top, jnp.max(scores, -1, keepdims=True))
        weights = jnp.exp(scores - higher)
        fade = jnp.exp(top - higher)
        total = total * fade + jnp.sum(weights, -1, keepdims=True)
        acc = acc * fade + jnp.dot(
            weights.astype(jnp.bfloat16), vs[part], preferred_element_type=jnp.float32)
        top = higher
    own = acc / total
    own_level = top + jnp.log(total)

    f_a = lambda i, s: remote(kva.at[s], kva.at[s], fa_send.at[i], fa_recv.at[i], sibling)
    f_b = lambda s: remote(kvb.at[s], kvb.at[s], fb_send, fb_recv, sibling)

    def forward_a(i):
        x_a(i, i * 2 + core).wait_recv()
        f_a(i, i * 2 + core).start()

    peers(wide, x, forward_a)
    near = (1 - y) * 2 + core
    y_b(near).wait_recv()
    f_b(near).start()
    peers(na, ia, lambda i: q_a(i, i).wait_recv())
    peers(nb, ib, lambda i: q_b(i, i).wait_recv())
    c_a(slot_a).wait_recv()
    c_b(slot_b).wait_recv()

    def attend(n, qbuf, kvbuf, obuf, lbuf):
        blocks = kvbuf.shape[0]
        lane = lax.broadcasted_iota(jnp.int32, (n * rows, depth), 1)
        levels = jnp.zeros((n * rows, depth), jnp.float32)
        for g in range(half):
            part = pl.ds(g * rows, rows)
            q = qbuf[:, part, :].astype(jnp.float32).reshape(n * rows, depth).astype(jnp.bfloat16)
            k = kvbuf[:, 0, g].reshape(blocks * count_p, depth)
            v = kvbuf[:, 1, g].reshape(blocks * count_p, depth)
            s = dot_nt(q, k) * scaling
            m = jnp.max(s, -1, keepdims=True)
            w = jnp.exp(s - m)
            t = jnp.sum(w, -1, keepdims=True)
            o = jnp.dot(w.astype(jnp.bfloat16), v, preferred_element_type=jnp.float32) / t
            obuf[:, part, :] = o.reshape(n, rows, depth).astype(jnp.bfloat16)
            levels = jnp.where(lane == g, m + jnp.log(t), levels)
        lbuf[...] = levels.reshape(n, rows, depth)

    o_a = lambda i, s: remote(oa.at[i], ra.at[s], oa_send.at[i], oa_recv.at[s], device_a(i))
    o_b = lambda i, s: remote(ob.at[i], rb.at[s], ob_send.at[i], ob_recv.at[s], device_b(i))
    l_a = lambda i, s: remote(la.at[i], sa.at[s], la_send.at[i], la_recv.at[s], device_a(i))
    l_b = lambda i, s: remote(lb.at[i], sb.at[s], lb_send.at[i], lb_recv.at[s], device_b(i))

    f_b(near).wait_recv()
    attend(nb, qb, kvb, ob, lb)

    def send_b(i):
        o_b(i, ib).start()
        l_b(i, ib).start()

    peers(nb, ib, send_b)
    rb[ib] = ob[ib]
    sb[ib] = lb[ib]
    peers(wide, x, lambda i: f_a(i, i * 2 + core).wait_recv())
    attend(na, qa, kva, oa, la)

    def send_a(i):
        o_a(i, ia).start()
        l_a(i, ia).start()

    peers(na, ia, send_a)
    ra[ia] = oa[ia]
    sa[ia] = la[ia]

    def merge(n, first, rbuf, sbuf):
        lane = lax.broadcasted_iota(jnp.int32, (rows, depth), 1)
        mine = jnp.zeros((rows, depth), jnp.float32)
        for g in range(half):
            at = (first + g) * rows
            mine = jnp.where(lane == g, own_level[at : at + rows], mine)
        levels = sbuf[...]
        most = jnp.maximum(jnp.max(levels, 0), mine)
        factor, factor_mine = jnp.exp(levels - most), jnp.exp(mine - most)
        inverse = 1.0 / (jnp.sum(factor, 0) + factor_mine)
        factor, factor_mine = factor * inverse, factor_mine * inverse
        for g in range(half):
            at = (first + g) * rows
            result = own[at : at + rows] * factor_mine[:, g : g + 1]
            outs = rbuf[:, g * rows : (g + 1) * rows, :].astype(jnp.float32)
            result += jnp.sum(outs * factor[:, :, g : g + 1], 0)
            out_ref[at : at + rows] = result.astype(jnp.bfloat16)

    def arrive_b(i):
        o_b(i, i).wait_recv()
        l_b(i, i).wait_recv()

    def arrive_a(i):
        o_a(i, i).wait_recv()
        l_a(i, i).wait_recv()

    peers(nb, ib, arrive_b)
    merge(nb, half, rb, sb)
    peers(na, ia, arrive_a)
    merge(na, 0, ra, sa)

    def sent_a(i):
        q_a(i, ia).wait_send()
        o_a(i, ia).wait_send()
        l_a(i, ia).wait_send()

    def sent_b(i):
        q_b(i, ib).wait_send()
        o_b(i, ib).wait_send()
        l_b(i, ib).wait_send()

    def sent_x(i):
        x_a(i, slot_a).wait_send()
        f_a(i, i * 2 + core).wait_send()

    peers(na, ia, sent_a)
    peers(nb, ib, sent_b)
    peers(wide, x, sent_x)
    y_b(slot_b).wait_send()
    f_b(near).wait_send()
    c_a(slot_a).wait_send()
    c_b(slot_b).wait_send()


def body(deep, wide, queries, prefix_keys, prefix_values, suffix_keys, suffix_values, lengths):
    _, new_tokens, heads, depth = queries.shape
    count_p, kv_heads, _ = prefix_keys.shape
    slots = suffix_keys.shape[1]
    group = heads // kv_heads
    rows, half = new_tokens * group, kv_heads // 2
    q = queries.reshape(new_tokens, kv_heads, group, depth).transpose(1, 0, 2, 3)
    q = q.reshape(2, half * rows, depth)
    prompt = jnp.stack([prefix_keys, prefix_values])
    prompt = prompt.reshape(2, count_p, 2, half, depth).transpose(2, 0, 3, 1, 4)
    na, nb = 2 * deep, deep * wide
    dma = pltpu.SemaphoreType.DMA
    bf, f32 = jnp.bfloat16, jnp.float32
    flat = slots * kv_heads
    span = flat // CHUNKS
    out = pl.pallas_call(
        functools.partial(kernel, (deep, wide, new_tokens, rows, half, count_p, depth, kv_heads)),
        out_shape=jax.ShapeDtypeStruct((kv_heads * rows, depth), bf),
        in_specs=[pl.BlockSpec(memory_space=pltpu.SMEM)] + [pl.BlockSpec(memory_space=pl.ANY)] * 4,
        out_specs=pl.BlockSpec(memory_space=pltpu.VMEM),
        scratch_shapes=[
            pltpu.VMEM((2, half * rows, depth), bf),
            pltpu.VMEM((flat, depth), bf),
            pltpu.VMEM((flat, depth), bf),
            pltpu.VMEM((kv_heads * rows, span), jnp.int32),
            pltpu.VMEM((na, half * rows, depth), bf),
            pltpu.VMEM((nb, half * rows, depth), bf),
            pltpu.VMEM((2 * wide, 2, half, count_p, depth), bf),
            pltpu.VMEM((4, 2, half, count_p, depth), bf),
            pltpu.VMEM((na, half * rows, depth), bf),
            pltpu.VMEM((nb, half * rows, depth), bf),
            pltpu.VMEM((na, rows, depth), f32),
            pltpu.VMEM((nb, rows, depth), f32),
            pltpu.VMEM((na, half * rows, depth), bf),
            pltpu.VMEM((nb, half * rows, depth), bf),
            pltpu.VMEM((na, rows, depth), f32),
            pltpu.VMEM((nb, rows, depth), f32),
            dma((2, CHUNKS)), dma((5,)), dma((na,)), dma((na,)), dma((nb,)), dma((nb,)),
            dma((2,)), dma((2,)), dma((wide,)), dma((wide,)), dma((wide,)), dma((wide,)), dma, dma,
            dma, dma, dma((na,)), dma((na,)), dma((nb,)), dma((nb,)),
            dma((na,)), dma((na,)), dma((nb,)), dma((nb,)),
        ],
        compiler_params=pltpu.CompilerParams(
            collective_id=0, has_side_effects=True, vmem_limit_bytes=48 * 1024 * 1024
        ),
    )(lengths, q, prompt, suffix_keys.reshape(flat, depth), suffix_values.reshape(flat, depth))
    out = out.reshape(kv_heads, new_tokens, group, depth).transpose(1, 0, 2, 3)
    return out.reshape(1, new_tokens, heads, depth)


def solution(mesh):
    deep, wide = mesh.shape["kv"] // 4, mesh.shape["batch"]
    return jax.shard_map(
        functools.partial(body, deep, wide),
        mesh=mesh,
        in_specs=(
            P(("kv", "batch"), None, None, None),
            P(("kv", "batch"), None, None),
            P(("kv", "batch"), None, None),
            P(("kv", "batch"), None, None, None),
            P(("kv", "batch"), None, None, None),
            P(("kv", "batch")),
        ),
        out_specs=P(("kv", "batch"), None, None, None),
        check_vma=False,
    )
```

```python
import functools

import jax
import jax.numpy as jnp
from jax import lax
from jax.experimental import pallas as pl
from jax.experimental.pallas import tpu as pltpu
from jax.sharding import PartitionSpec as P

QUERY_SCALE = 144
MESH = pl.DeviceIdType.MESH
masked_score = -1e30
CHUNKS = 8


def dot_nt(a, b):
    return lax.dot_general(a, b, (((1,), (1,)), ((), ())), preferred_element_type=jnp.float32)


def kernel(
    sizes, length, q_hbm, pk_hbm, pv_hbm, sk_hbm, sv_hbm, out_ref,
    qs, merged, pk, pv, ks, vs, times, qa, qb, kva, kvb, oa, ob, la, lb, ra, rb, sa, sb,
    suffix_sem, local_sem, qa_send, qa_recv, qb_send, qb_recv,
    core_send, core_recv, xa_send, xa_recv, fa_send, fa_recv, yb_send, yb_recv,
    fb_send, fb_recv, oa_send, oa_recv, ob_send, ob_recv,
    la_send, la_recv, lb_send, lb_recv,
):
    deep, wide, new_tokens, rows, half, count_p, depth, kv_heads = sizes
    kv, x = lax.axis_index("kv"), lax.axis_index("batch")
    core, zy = kv % 2, kv // 2
    y, z = zy % 2, zy // 2
    na, nb = 2 * deep, deep * wide
    ia, ib = zy, z * wide + x
    scaling = QUERY_SCALE ** (-0.5)

    def device_a(i):
        return (i * 2 + core, x)

    def device_b(i):
        return ((i // wide * 2 + y) * 2 + core, i % wide)

    sibling = (kv + 1 - 2 * core, x)
    slot_a, slot_b = x * 2 + core, y * 2 + core

    locals_ = [
        pltpu.make_async_copy(q_hbm, qs, local_sem.at[0]),
        pltpu.make_async_copy(pk_hbm, pk, local_sem.at[1]),
        pltpu.make_async_copy(pv_hbm, pv, local_sem.at[2]),
    ]
    for copy in locals_:
        copy.start()
    span = ks.shape[0] // CHUNKS
    loads = []
    for c in range(CHUNKS):
        part = pl.ds(c * span, span)
        loads.append((
            pltpu.make_async_copy(sk_hbm.at[part], ks.at[part], suffix_sem.at[0, c]),
            pltpu.make_async_copy(sv_hbm.at[part], vs.at[part], suffix_sem.at[1, c]),
        ))
        for copy in loads[-1]:
            copy.start()

    barrier = pltpu.get_barrier_semaphore()

    def peers(n, me, act):
        def step(k, carry):
            act(lax.rem(me + k, n))
            return carry

        lax.fori_loop(1, n, step, 0, unroll=n <= 16)

    def greet(device):
        pl.semaphore_signal(barrier, inc=1, device_id=device, device_id_type=MESH)

    greet(sibling)
    peers(na, ia, lambda i: greet(device_a(i)))
    peers(nb, ib, lambda i: greet(device_b(i)))
    total_rows = kv_heads * rows
    group = rows // new_tokens
    ordered = lax.broadcasted_iota(jnp.int32, (total_rows, total_rows), 0)
    natural = lax.broadcasted_iota(jnp.int32, (total_rows, total_rows), 1)
    token_of = ordered % rows // group
    source = token_of * (kv_heads * group) + ordered // rows * group + ordered % group
    swap = jnp.where(source == natural, 1.0, 0.0).astype(jnp.bfloat16)
    for copy in locals_:
        copy.wait()
    queries = jnp.dot(swap, qs[...], preferred_element_type=jnp.float32).astype(jnp.bfloat16)
    qa[ia] = queries[: half * rows]
    qb[ib] = queries[half * rows :]
    for index, prompt in enumerate((pk, pv)):
        block = jnp.swapaxes(prompt[...].astype(jnp.float32), 0, 1).astype(jnp.bfloat16)
        kva[slot_a, index] = block[:half]
        kvb[slot_b, index] = block[half:]
    pl.semaphore_wait(barrier, na + nb - 1)

    def remote(src, dst, send, recv, device):
        return pltpu.make_async_remote_copy(
            src_ref=src, dst_ref=dst, send_sem=send, recv_sem=recv,
            device_id=device, device_id_type=MESH,
        )

    q_a = lambda i, s: remote(qa.at[s], qa.at[s], qa_send.at[i], qa_recv.at[s], device_a(i))
    q_b = lambda i, s: remote(qb.at[s], qb.at[s], qb_send.at[i], qb_recv.at[s], device_b(i))
    peers(na, ia, lambda i: q_a(i, ia).start())
    peers(nb, ib, lambda i: q_b(i, ib).start())
    x_a = lambda i, s: remote(
        kva.at[s], kva.at[s], xa_send.at[i], xa_recv.at[s // 2], (kv, i))
    peers(wide, x, lambda i: x_a(i, slot_a).start())
    y_b = lambda s: remote(
        kvb.at[s], kvb.at[s], yb_send, yb_recv, ((z * 2 + 1 - y) * 2 + core, x))
    y_b(slot_b).start()
    c_a = lambda s: remote(kva.at[s], kva.at[s], core_send.at[0], core_recv.at[0], sibling)
    c_b = lambda s: remote(kvb.at[s], kvb.at[s], core_send.at[1], core_recv.at[1], sibling)
    c_a(slot_a).start()
    c_b(slot_b).start()

    row = lax.broadcasted_iota(jnp.int32, (total_rows, span), 0)
    col = lax.broadcasted_iota(jnp.int32, (total_rows, span), 1)
    times[...] = jnp.where(row // rows == col % kv_heads, col // kv_heads, 2 ** 30)
    token = lax.broadcasted_iota(jnp.int32, (total_rows, 1), 0) % rows // group
    limit = length[0] - new_tokens + 1 + token
    top = jnp.full((total_rows, 1), masked_score, jnp.float32)
    total = jnp.zeros((total_rows, 1), jnp.float32)
    acc = jnp.zeros((total_rows, depth), jnp.float32)
    for c in range(CHUNKS):
        for copy in loads[c]:
            copy.wait()
        part = pl.ds(c * span, span)
        scores = dot_nt(queries, ks[part]) * scaling
        scores = jnp.where(times[...] < limit - c * (span // kv_heads), scores, masked_score)
        higher = jnp.maximum(top, jnp.max(scores, -1, keepdims=True))
        weights = jnp.exp(scores - higher)
        fade = jnp.exp(top - higher)
        total = total * fade + jnp.sum(weights, -1, keepdims=True)
        acc = acc * fade + jnp.dot(
            weights.astype(jnp.bfloat16), vs[part], preferred_element_type=jnp.float32)
        top = higher
    own = acc / total
    own_level = top + jnp.log(total)

    f_a = lambda i, s: remote(kva.at[s], kva.at[s], fa_send.at[i], fa_recv.at[i], sibling)
    f_b = lambda s: remote(kvb.at[s], kvb.at[s], fb_send, fb_recv, sibling)

    def forward_a(i):
        x_a(i, i * 2 + core).wait_recv()
        f_a(i, i * 2 + core).start()

    peers(wide, x, forward_a)
    near = (1 - y) * 2 + core
    y_b(near).wait_recv()
    f_b(near).start()
    peers(na, ia, lambda i: q_a(i, i).wait_recv())
    peers(nb, ib, lambda i: q_b(i, i).wait_recv())
    c_a(slot_a).wait_recv()
    c_b(slot_b).wait_recv()

    def attend(n, qbuf, kvbuf, obuf, lbuf):
        blocks = kvbuf.shape[0]
        lane = lax.broadcasted_iota(jnp.int32, (n * rows, depth), 1)
        levels = jnp.zeros((n * rows, depth), jnp.float32)
        for g in range(half):
            part = pl.ds(g * rows, rows)
            q = qbuf[:, part, :].astype(jnp.float32).reshape(n * rows, depth).astype(jnp.bfloat16)
            k = kvbuf[:, 0, g].reshape(blocks * count_p, depth)
            v = kvbuf[:, 1, g].reshape(blocks * count_p, depth)
            s = dot_nt(q, k) * scaling
            m = jnp.max(s, -1, keepdims=True)
            w = jnp.exp(s - m)
            t = jnp.sum(w, -1, keepdims=True)
            o = jnp.dot(w.astype(jnp.bfloat16), v, preferred_element_type=jnp.float32) / t
            obuf[:, part, :] = o.reshape(n, rows, depth).astype(jnp.bfloat16)
            levels = jnp.where(lane == g, m + jnp.log(t), levels)
        lbuf[...] = levels.reshape(n, rows, depth)

    o_a = lambda i, s: remote(oa.at[i], ra.at[s], oa_send.at[i], oa_recv.at[s], device_a(i))
    o_b = lambda i, s: remote(ob.at[i], rb.at[s], ob_send.at[i], ob_recv.at[s], device_b(i))
    l_a = lambda i, s: remote(la.at[i], sa.at[s], la_send.at[i], la_recv.at[s], device_a(i))
    l_b = lambda i, s: remote(lb.at[i], sb.at[s], lb_send.at[i], lb_recv.at[s], device_b(i))

    f_b(near).wait_recv()
    attend(nb, qb, kvb, ob, lb)

    def send_b(i):
        o_b(i, ib).start()
        l_b(i, ib).start()

    peers(nb, ib, send_b)
    rb[ib] = ob[ib]
    sb[ib] = lb[ib]
    peers(wide, x, lambda i: f_a(i, i * 2 + core).wait_recv())
    attend(na, qa, kva, oa, la)

    def send_a(i):
        o_a(i, ia).start()
        l_a(i, ia).start()

    peers(na, ia, send_a)
    ra[ia] = oa[ia]
    sa[ia] = la[ia]

    def merge(n, first, rbuf, sbuf):
        lane = lax.broadcasted_iota(jnp.int32, (rows, depth), 1)
        mine = jnp.zeros((rows, depth), jnp.float32)
        for g in range(half):
            at = (first + g) * rows
            mine = jnp.where(lane == g, own_level[at : at + rows], mine)
        levels = sbuf[...]
        most = jnp.maximum(jnp.max(levels, 0), mine)
        factor, factor_mine = jnp.exp(levels - most), jnp.exp(mine - most)
        inverse = 1.0 / (jnp.sum(factor, 0) + factor_mine)
        factor, factor_mine = factor * inverse, factor_mine * inverse
        for g in range(half):
            at = (first + g) * rows
            result = own[at : at + rows] * factor_mine[:, g : g + 1]
            outs = rbuf[:, g * rows : (g + 1) * rows, :].astype(jnp.float32)
            result += jnp.sum(outs * factor[:, :, g : g + 1], 0)
            merged[at : at + rows] = result

    def arrive_b(i):
        o_b(i, i).wait_recv()
        l_b(i, i).wait_recv()

    def arrive_a(i):
        o_a(i, i).wait_recv()
        l_a(i, i).wait_recv()

    peers(nb, ib, arrive_b)
    merge(nb, half, rb, sb)
    peers(na, ia, arrive_a)
    merge(na, 0, ra, sa)
    out_ref[...] = lax.dot_general(
        swap, merged[...].astype(jnp.bfloat16), (((0,), (0,)), ((), ())),
        preferred_element_type=jnp.float32).astype(jnp.bfloat16)

    def sent_a(i):
        q_a(i, ia).wait_send()
        o_a(i, ia).wait_send()
        l_a(i, ia).wait_send()

    def sent_b(i):
        q_b(i, ib).wait_send()
        o_b(i, ib).wait_send()
        l_b(i, ib).wait_send()

    def sent_x(i):
        x_a(i, slot_a).wait_send()
        f_a(i, i * 2 + core).wait_send()

    peers(na, ia, sent_a)
    peers(nb, ib, sent_b)
    peers(wide, x, sent_x)
    y_b(slot_b).wait_send()
    f_b(near).wait_send()
    c_a(slot_a).wait_send()
    c_b(slot_b).wait_send()


def body(deep, wide, queries, prefix_keys, prefix_values, suffix_keys, suffix_values, lengths):
    _, new_tokens, heads, depth = queries.shape
    count_p, kv_heads, _ = prefix_keys.shape
    slots = suffix_keys.shape[1]
    group = heads // kv_heads
    rows, half = new_tokens * group, kv_heads // 2
    q = queries.reshape(new_tokens * heads, depth)
    na, nb = 2 * deep, deep * wide
    dma = pltpu.SemaphoreType.DMA
    bf, f32 = jnp.bfloat16, jnp.float32
    flat = slots * kv_heads
    span = flat // CHUNKS
    out = pl.pallas_call(
        functools.partial(kernel, (deep, wide, new_tokens, rows, half, count_p, depth, kv_heads)),
        out_shape=jax.ShapeDtypeStruct((kv_heads * rows, depth), bf),
        in_specs=[pl.BlockSpec(memory_space=pltpu.SMEM)] + [pl.BlockSpec(memory_space=pltpu.HBM)] * 5,
        out_specs=pl.BlockSpec(memory_space=pltpu.VMEM),
        scratch_shapes=[
            pltpu.VMEM((kv_heads * rows, depth), bf),
            pltpu.VMEM((kv_heads * rows, depth), f32),
            pltpu.VMEM((count_p, kv_heads, depth), bf),
            pltpu.VMEM((count_p, kv_heads, depth), bf),
            pltpu.VMEM((flat, depth), bf),
            pltpu.VMEM((flat, depth), bf),
            pltpu.VMEM((kv_heads * rows, span), jnp.int32),
            pltpu.VMEM((na, half * rows, depth), bf),
            pltpu.VMEM((nb, half * rows, depth), bf),
            pltpu.VMEM((2 * wide, 2, half, count_p, depth), bf),
            pltpu.VMEM((4, 2, half, count_p, depth), bf),
            pltpu.VMEM((na, half * rows, depth), bf),
            pltpu.VMEM((nb, half * rows, depth), bf),
            pltpu.VMEM((na, rows, depth), f32),
            pltpu.VMEM((nb, rows, depth), f32),
            pltpu.VMEM((na, half * rows, depth), bf),
            pltpu.VMEM((nb, half * rows, depth), bf),
            pltpu.VMEM((na, rows, depth), f32),
            pltpu.VMEM((nb, rows, depth), f32),
            dma((2, CHUNKS)), dma((3,)), dma((na,)), dma((na,)), dma((nb,)), dma((nb,)),
            dma((2,)), dma((2,)), dma((wide,)), dma((wide,)), dma((wide,)), dma((wide,)), dma, dma,
            dma, dma, dma((na,)), dma((na,)), dma((nb,)), dma((nb,)),
            dma((na,)), dma((na,)), dma((nb,)), dma((nb,)),
        ],
        compiler_params=pltpu.CompilerParams(
            collective_id=0, has_side_effects=True, vmem_limit_bytes=67043328
        ),
    )(lengths, q, prefix_keys, prefix_values, suffix_keys.reshape(flat, depth), suffix_values.reshape(flat, depth))
    return out.reshape(1, new_tokens, heads, depth)


def solution(mesh):
    deep, wide = mesh.shape["kv"] // 4, mesh.shape["batch"]
    return jax.shard_map(
        functools.partial(body, deep, wide),
        mesh=mesh,
        in_specs=(
            P(("kv", "batch"), None, None, None),
            P(("kv", "batch"), None, None),
            P(("kv", "batch"), None, None),
            P(("kv", "batch"), None, None, None),
            P(("kv", "batch"), None, None, None),
            P(("kv", "batch")),
        ),
        out_specs=P(("kv", "batch"), None, None, None),
        check_vma=False,
    )
```

```python
import functools

import jax
import jax.numpy as jnp
from jax import lax
from jax.experimental import pallas as pl
from jax.experimental.pallas import tpu as pltpu
from jax.sharding import PartitionSpec as P

QUERY_SCALE = 144
MESH = pl.DeviceIdType.MESH
masked_score = -1e30
CHUNKS = 8


def dot_nt(a, b):
    return lax.dot_general(a, b, (((1,), (1,)), ((), ())), preferred_element_type=jnp.float32)


def kernel(
    sizes, length, q_hbm, pk_hbm, pv_hbm, sk_hbm, sv_hbm, out_ref,
    qs, merged, pk, pv, ks, vs, times, qa, qb, kva, kvb, oa, ob, la, lb, ra, rb, sa, sb,
    suffix_sem, local_sem, qa_send, qa_recv, qb_send, qb_recv,
    core_send, core_recv, xa_send, xa_recv, fa_send, fa_recv, yb_send, yb_recv,
    fb_send, fb_recv, oa_send, oa_recv, ob_send, ob_recv,
    la_send, la_recv, lb_send, lb_recv,
):
    deep, wide, new_tokens, rows, half, count_p, depth, kv_heads = sizes
    kv, x = lax.axis_index("kv"), lax.axis_index("batch")
    core, zy = kv % 2, kv // 2
    y, z = zy % 2, zy // 2
    na, nb = 2 * deep, deep * wide
    ia, ib = zy, z * wide + x
    scaling = QUERY_SCALE ** (-0.5)

    def device_a(i):
        return (i * 2 + core, x)

    def device_b(i):
        return ((i // wide * 2 + y) * 2 + core, i % wide)

    sibling = (kv + 1 - 2 * core, x)
    slot_a, slot_b = x * 2 + core, y * 2 + core

    locals_ = [
        pltpu.make_async_copy(q_hbm, qs, local_sem.at[0]),
        pltpu.make_async_copy(pk_hbm, pk, local_sem.at[1]),
        pltpu.make_async_copy(pv_hbm, pv, local_sem.at[2]),
    ]
    for copy in locals_:
        copy.start()

    barrier = pltpu.get_barrier_semaphore()

    def peers(n, me, act):
        def step(k, carry):
            act(lax.rem(me + k, n))
            return carry

        lax.fori_loop(1, n, step, 0, unroll=n <= 16)

    def greet(device):
        pl.semaphore_signal(barrier, inc=1, device_id=device, device_id_type=MESH)

    greet(sibling)
    peers(na, ia, lambda i: greet(device_a(i)))
    peers(nb, ib, lambda i: greet(device_b(i)))
    total_rows = kv_heads * rows
    group = rows // new_tokens
    ordered = lax.broadcasted_iota(jnp.int32, (total_rows, total_rows), 0)
    natural = lax.broadcasted_iota(jnp.int32, (total_rows, total_rows), 1)
    token_of = ordered % rows // group
    source = token_of * (kv_heads * group) + ordered // rows * group + ordered % group
    swap = jnp.where(source == natural, 1.0, 0.0).astype(jnp.bfloat16)
    for copy in locals_:
        copy.wait()
    queries = jnp.dot(swap, qs[...], preferred_element_type=jnp.float32).astype(jnp.bfloat16)
    qa[ia] = queries[: half * rows]
    qb[ib] = queries[half * rows :]
    for index, prompt in enumerate((pk, pv)):
        block = jnp.swapaxes(prompt[...].astype(jnp.float32), 0, 1).astype(jnp.bfloat16)
        kva[slot_a, index] = block[:half]
        kvb[slot_b, index] = block[half:]
    pl.semaphore_wait(barrier, na + nb - 1)

    def remote(src, dst, send, recv, device):
        return pltpu.make_async_remote_copy(
            src_ref=src, dst_ref=dst, send_sem=send, recv_sem=recv,
            device_id=device, device_id_type=MESH,
        )

    q_a = lambda i, s: remote(qa.at[s], qa.at[s], qa_send.at[i], qa_recv.at[s], device_a(i))
    q_b = lambda i, s: remote(qb.at[s], qb.at[s], qb_send.at[i], qb_recv.at[s], device_b(i))
    peers(na, ia, lambda i: q_a(i, ia).start())
    peers(nb, ib, lambda i: q_b(i, ib).start())
    x_a = lambda i, s: remote(
        kva.at[s], kva.at[s], xa_send.at[i], xa_recv.at[s // 2], (kv, i))
    peers(wide, x, lambda i: x_a(i, slot_a).start())
    y_b = lambda s: remote(
        kvb.at[s], kvb.at[s], yb_send, yb_recv, ((z * 2 + 1 - y) * 2 + core, x))
    y_b(slot_b).start()
    c_a = lambda s: remote(kva.at[s], kva.at[s], core_send.at[0], core_recv.at[0], sibling)
    c_b = lambda s: remote(kvb.at[s], kvb.at[s], core_send.at[1], core_recv.at[1], sibling)
    c_a(slot_a).start()
    c_b(slot_b).start()

    span = ks.shape[0] // CHUNKS
    loads = []
    for c in range(CHUNKS):
        part = pl.ds(c * span, span)
        loads.append((
            pltpu.make_async_copy(sk_hbm.at[part], ks.at[part], suffix_sem.at[0, c]),
            pltpu.make_async_copy(sv_hbm.at[part], vs.at[part], suffix_sem.at[1, c]),
        ))
        for copy in loads[-1]:
            copy.start()

    row = lax.broadcasted_iota(jnp.int32, (total_rows, span), 0)
    col = lax.broadcasted_iota(jnp.int32, (total_rows, span), 1)
    times[...] = jnp.where(row // rows == col % kv_heads, col // kv_heads, 2 ** 30)
    token = lax.broadcasted_iota(jnp.int32, (total_rows, 1), 0) % rows // group
    limit = length[0] - new_tokens + 1 + token
    top = jnp.full((total_rows, 1), masked_score, jnp.float32)
    total = jnp.zeros((total_rows, 1), jnp.float32)
    acc = jnp.zeros((total_rows, depth), jnp.float32)
    for c in range(CHUNKS):
        for copy in loads[c]:
            copy.wait()
        part = pl.ds(c * span, span)
        scores = dot_nt(queries, ks[part]) * scaling
        scores = jnp.where(times[...] < limit - c * (span // kv_heads), scores, masked_score)
        higher = jnp.maximum(top, jnp.max(scores, -1, keepdims=True))
        weights = jnp.exp(scores - higher)
        fade = jnp.exp(top - higher)
        total = total * fade + jnp.sum(weights, -1, keepdims=True)
        acc = acc * fade + jnp.dot(
            weights.astype(jnp.bfloat16), vs[part], preferred_element_type=jnp.float32)
        top = higher
    own = acc / total
    own_level = top + jnp.log(total)

    f_a = lambda i, s: remote(kva.at[s], kva.at[s], fa_send.at[i], fa_recv.at[i], sibling)
    f_b = lambda s: remote(kvb.at[s], kvb.at[s], fb_send, fb_recv, sibling)

    def forward_a(i):
        x_a(i, i * 2 + core).wait_recv()
        f_a(i, i * 2 + core).start()

    peers(wide, x, forward_a)
    near = (1 - y) * 2 + core
    y_b(near).wait_recv()
    f_b(near).start()
    peers(na, ia, lambda i: q_a(i, i).wait_recv())
    peers(nb, ib, lambda i: q_b(i, i).wait_recv())
    c_a(slot_a).wait_recv()
    c_b(slot_b).wait_recv()

    def attend(n, qbuf, kvbuf, obuf, lbuf):
        blocks = kvbuf.shape[0]
        lane = lax.broadcasted_iota(jnp.int32, (n * rows, depth), 1)
        levels = jnp.zeros((n * rows, depth), jnp.float32)
        for g in range(half):
            part = pl.ds(g * rows, rows)
            q = qbuf[:, part, :].astype(jnp.float32).reshape(n * rows, depth).astype(jnp.bfloat16)
            k = kvbuf[:, 0, g].reshape(blocks * count_p, depth)
            v = kvbuf[:, 1, g].reshape(blocks * count_p, depth)
            s = dot_nt(q, k) * scaling
            m = jnp.max(s, -1, keepdims=True)
            w = jnp.exp(s - m)
            t = jnp.sum(w, -1, keepdims=True)
            o = jnp.dot(w.astype(jnp.bfloat16), v, preferred_element_type=jnp.float32) / t
            obuf[:, part, :] = o.reshape(n, rows, depth).astype(jnp.bfloat16)
            levels = jnp.where(lane == g, m + jnp.log(t), levels)
        lbuf[...] = levels.reshape(n, rows, depth)

    o_a = lambda i, s: remote(oa.at[i], ra.at[s], oa_send.at[i], oa_recv.at[s], device_a(i))
    o_b = lambda i, s: remote(ob.at[i], rb.at[s], ob_send.at[i], ob_recv.at[s], device_b(i))
    l_a = lambda i, s: remote(la.at[i], sa.at[s], la_send.at[i], la_recv.at[s], device_a(i))
    l_b = lambda i, s: remote(lb.at[i], sb.at[s], lb_send.at[i], lb_recv.at[s], device_b(i))

    f_b(near).wait_recv()
    attend(nb, qb, kvb, ob, lb)

    def send_b(i):
        o_b(i, ib).start()
        l_b(i, ib).start()

    peers(nb, ib, send_b)
    rb[ib] = ob[ib]
    sb[ib] = lb[ib]
    peers(wide, x, lambda i: f_a(i, i * 2 + core).wait_recv())
    attend(na, qa, kva, oa, la)

    def send_a(i):
        o_a(i, ia).start()
        l_a(i, ia).start()

    peers(na, ia, send_a)
    ra[ia] = oa[ia]
    sa[ia] = la[ia]

    def merge(n, first, rbuf, sbuf):
        lane = lax.broadcasted_iota(jnp.int32, (rows, depth), 1)
        mine = jnp.zeros((rows, depth), jnp.float32)
        for g in range(half):
            at = (first + g) * rows
            mine = jnp.where(lane == g, own_level[at : at + rows], mine)
        levels = sbuf[...]
        most = jnp.maximum(jnp.max(levels, 0), mine)
        factor, factor_mine = jnp.exp(levels - most), jnp.exp(mine - most)
        inverse = 1.0 / (jnp.sum(factor, 0) + factor_mine)
        factor, factor_mine = factor * inverse, factor_mine * inverse
        for g in range(half):
            at = (first + g) * rows
            result = own[at : at + rows] * factor_mine[:, g : g + 1]
            outs = rbuf[:, g * rows : (g + 1) * rows, :].astype(jnp.float32)
            result += jnp.sum(outs * factor[:, :, g : g + 1], 0)
            merged[at : at + rows] = result

    def arrive_b(i):
        o_b(i, i).wait_recv()
        l_b(i, i).wait_recv()

    def arrive_a(i):
        o_a(i, i).wait_recv()
        l_a(i, i).wait_recv()

    peers(nb, ib, arrive_b)
    merge(nb, half, rb, sb)
    peers(na, ia, arrive_a)
    merge(na, 0, ra, sa)
    out_ref[...] = lax.dot_general(
        swap, merged[...].astype(jnp.bfloat16), (((0,), (0,)), ((), ())),
        preferred_element_type=jnp.float32).astype(jnp.bfloat16)

    def sent_a(i):
        q_a(i, ia).wait_send()
        o_a(i, ia).wait_send()
        l_a(i, ia).wait_send()

    def sent_b(i):
        q_b(i, ib).wait_send()
        o_b(i, ib).wait_send()
        l_b(i, ib).wait_send()

    def sent_x(i):
        x_a(i, slot_a).wait_send()
        f_a(i, i * 2 + core).wait_send()

    peers(na, ia, sent_a)
    peers(nb, ib, sent_b)
    peers(wide, x, sent_x)
    y_b(slot_b).wait_send()
    f_b(near).wait_send()
    c_a(slot_a).wait_send()
    c_b(slot_b).wait_send()


def body(deep, wide, queries, prefix_keys, prefix_values, suffix_keys, suffix_values, lengths):
    _, new_tokens, heads, depth = queries.shape
    count_p, kv_heads, _ = prefix_keys.shape
    slots = suffix_keys.shape[1]
    group = heads // kv_heads
    rows, half = new_tokens * group, kv_heads // 2
    q = queries.reshape(new_tokens * heads, depth)
    na, nb = 2 * deep, deep * wide
    dma = pltpu.SemaphoreType.DMA
    bf, f32 = jnp.bfloat16, jnp.float32
    flat = slots * kv_heads
    span = flat // CHUNKS
    out = pl.pallas_call(
        functools.partial(kernel, (deep, wide, new_tokens, rows, half, count_p, depth, kv_heads)),
        out_shape=jax.ShapeDtypeStruct((kv_heads * rows, depth), bf),
        in_specs=[pl.BlockSpec(memory_space=pltpu.SMEM)] + [pl.BlockSpec(memory_space=pltpu.HBM)] * 5,
        out_specs=pl.BlockSpec(memory_space=pltpu.VMEM),
        scratch_shapes=[
            pltpu.VMEM((kv_heads * rows, depth), bf),
            pltpu.VMEM((kv_heads * rows, depth), f32),
            pltpu.VMEM((count_p, kv_heads, depth), bf),
            pltpu.VMEM((count_p, kv_heads, depth), bf),
            pltpu.VMEM((flat, depth), bf),
            pltpu.VMEM((flat, depth), bf),
            pltpu.VMEM((kv_heads * rows, span), jnp.int32),
            pltpu.VMEM((na, half * rows, depth), bf),
            pltpu.VMEM((nb, half * rows, depth), bf),
            pltpu.VMEM((2 * wide, 2, half, count_p, depth), bf),
            pltpu.VMEM((4, 2, half, count_p, depth), bf),
            pltpu.VMEM((na, half * rows, depth), bf),
            pltpu.VMEM((nb, half * rows, depth), bf),
            pltpu.VMEM((na, rows, depth), f32),
            pltpu.VMEM((nb, rows, depth), f32),
            pltpu.VMEM((na, half * rows, depth), bf),
            pltpu.VMEM((nb, half * rows, depth), bf),
            pltpu.VMEM((na, rows, depth), f32),
            pltpu.VMEM((nb, rows, depth), f32),
            dma((2, CHUNKS)), dma((3,)), dma((na,)), dma((na,)), dma((nb,)), dma((nb,)),
            dma((2,)), dma((2,)), dma((wide,)), dma((wide,)), dma((wide,)), dma((wide,)), dma, dma,
            dma, dma, dma((na,)), dma((na,)), dma((nb,)), dma((nb,)),
            dma((na,)), dma((na,)), dma((nb,)), dma((nb,)),
        ],
        compiler_params=pltpu.CompilerParams(
            collective_id=0, has_side_effects=True, vmem_limit_bytes=67043328
        ),
    )(lengths, q, prefix_keys, prefix_values, suffix_keys.reshape(flat, depth), suffix_values.reshape(flat, depth))
    return out.reshape(1, new_tokens, heads, depth)


def solution(mesh):
    deep, wide = mesh.shape["kv"] // 4, mesh.shape["batch"]
    return jax.shard_map(
        functools.partial(body, deep, wide),
        mesh=mesh,
        in_specs=(
            P(("kv", "batch"), None, None, None),
            P(("kv", "batch"), None, None),
            P(("kv", "batch"), None, None),
            P(("kv", "batch"), None, None, None),
            P(("kv", "batch"), None, None, None),
            P(("kv", "batch")),
        ),
        out_specs=P(("kv", "batch"), None, None, None),
        check_vma=False,
    )
```
